32 devices in a mesh: shuf: 8 (over z, y), rep: 4 (over x, core).
Axes of the slice: x: 2, y: 2, z: 4, core: 2. Of those that a mesh axis runs over, the one named last changes fastest.
Arguments:
- values: bfloat16 [65536, 1024], P('shuf', 'rep')
- subgroup: int32 [512], P('shuf'), may hold values from 0 to 31
- owners: int32 [512, 1], P('shuf'), may hold values from 0 to 7; in each aligned block of 64 rows (0 to 63, 64 to 127, ...) at most 16 rows name the same one
- col_gain: float32 [1024], P('rep'), may hold values from 0.5 to 1.5
- col_bias: float32 [1024], P('rep'), may hold values from -3 to 3
- out_weight: bfloat16 [1024, 1024], P('rep'), may hold values from -0.1875 to 0.1875
Outputs:
- projected: bfloat16 [65536, 1024], P(('shuf', 'rep'))
The draws below stay inside these ranges and needn't reach their ends.
Inputs may be any that keep to these rules, and one draw needn't show every extreme that they name: `owners`: among the tiles of one index of shuf no owner is named more than 16 times, a bound that some block reaches.
All inputs are finite; a program needn't handle non-finite values.
Results may differ from the reference program's by a relative error of at most 0.015.
Values may be sent and summed in bfloat16 or wider, within the bound.
A program may use at most 64 MiB of HBM per device.

```python
import math
import jax
import jax.numpy as jnp
import numpy as np
from jax import lax

TILE = 128
TILES_DEV = 64
COLS = 1024
OUT = 1024
GRP_DEV = 32
PRIOR = 256
ROWS_DEV = 8192
TILES = 512
ROWS = 65536
CAP = 16
N_SHUF = 8
N_REP = 4


def draw_values(key, part):
    keys = jax.random.split(jax.random.fold_in(key, 11), 7)
    blocks = ROWS // ROWS_DEV
    place = jnp.arange(ROWS, dtype=jnp.float32).reshape(TILES, TILE, 1) / float(ROWS)
    rough = jax.random.uniform(keys[0], (TILES, TILE, 1), minval=0.7, maxval=1.4)
    row_scale = jnp.exp(jnp.log(3.0) * place) * rough
    shift = 1.5 * jax.random.normal(keys[4], (blocks, 1, COLS))
    shift_rows = jnp.repeat(shift, TILES_DEV, axis=0)
    chosen = jax.random.bernoulli(keys[5], 0.5, (TILES, 1, COLS))
    stretch = jnp.exp(jax.random.uniform(keys[6], (TILES, 1, COLS), minval=-0.6, maxval=0.6))
    factor = jnp.where(chosen, stretch, 1.0)
    col_scale = jnp.exp(jax.random.uniform(keys[1], (1, 1, COLS), minval=0.0, maxval=jnp.log(10.0)))
    noise = jax.random.normal(keys[2], (TILES, TILE, COLS))
    offset = jax.random.normal(keys[3], (1, 1, COLS)) * (0.5 + 2.0 * place)
    drawn = col_scale * (offset + shift_rows + row_scale * noise * factor)
    return drawn.reshape(ROWS, COLS).astype(jnp.bfloat16)


def set_ends(values, stream_key, low, largest):
    spot = [jax.random.randint(jax.random.fold_in(stream_key, axis), (), 0, length) for axis, length in enumerate(values.shape)]
    widest = values.shape.index(max(values.shape))
    beside = spot[:widest] + [(spot[widest] + 1) % values.shape[widest]] + spot[widest + 1:]
    return values.at[tuple(spot)].set(low).at[tuple(beside)].set(largest)


def level_of(own_key, dims, pieces, smallest, high):
    gain, own = 1.0, jax.random.fold_in(own_key, 6)
    for axis_at, parts in pieces:
        heights = jnp.exp(jax.random.uniform(jax.random.fold_in(own, axis_at), (parts,), jnp.float32, smallest / len(pieces), high / len(pieces)))
        gain = gain * jnp.repeat(heights, dims[axis_at] // parts).reshape([-1 if axis == axis_at else 1 for axis in range(len(dims))])
    return gain


def assign_block(key, own, number, rows, amount, top, most, slope):
    sequence = jax.random.permutation(key, amount)
    heavy_load, ordinary = load_shares(amount, rows * top, most, slope, True), load_shares(amount, rows * top, most, slope, False)
    places = jnp.arange(amount)

    def named(tallies, offset_by):
        used = int((tallies > 0).sum())
        fixed = max(1, used // 4)
        passed = fixed + (places - fixed + offset_by * (used - fixed)) % max(1, amount - fixed)
        return jnp.zeros((amount,), jnp.int32).at[sequence[jnp.where(places < fixed, places, passed)]].set(jnp.asarray(tallies, jnp.int32))

    tallies = jnp.where(number % 4 == 0, named(heavy_load, number // 4), named(ordinary, number - number // 4 - 1))
    mixed = jax.random.permutation(jax.random.fold_in(own, 3), amount)
    source_of, sink = mixed[0:amount // 2 * 2:2], mixed[1:amount // 2 * 2:2]
    margin = jnp.minimum(tallies[source_of] - 1, most - tallies[sink]) // 2
    margin = jnp.where((source_of == sequence[0]) | (sink == sequence[0]) | (tallies[sink] == 0), 0, jnp.maximum(margin, 0))
    passed = jax.random.randint(jax.random.fold_in(own, 4), (amount // 2,), 0, 1 << 20) % (margin + 1)
    tallies = tallies.at[source_of].add(-passed).at[sink].add(passed)
    labels = jnp.searchsorted(jnp.cumsum(tallies), jnp.arange(rows * top), side="right").astype(jnp.int32)
    listing = labels.reshape(top, rows).T
    listing = listing[jax.random.permutation(jax.random.fold_in(own, 1), rows)]
    offset_by = jax.random.randint(jax.random.fold_in(own, 2), (rows, 1), 0, top)
    return jnp.take_along_axis(listing, (jnp.arange(top)[None, :] + offset_by) % top, axis=1)


def load_shares(count, total, limit, slope, full):
    portions = [(1 << 20) // math.isqrt(rank ** slope) + 1 for rank in range(1, count + 1)]
    largest = limit if full else min(limit, max(-(-total // count), total * portions[0] // sum(portions)))
    least = 1 if total - largest >= count - 1 else 0
    counts, surplus = [largest] + [least] * (count - 1), total - largest - least * (count - 1)
    while surplus > 0:
        movable = [i for i in range(1, count) if counts[i] < largest] or [i for i in range(1, count) if counts[i] < limit]
        whole, remaining = sum([portions[i] for i in movable]), surplus
        for i in movable:
            more = min(limit - counts[i], max(1, remaining * portions[i] // whole), surplus)
            counts[i] = counts[i] + more
            surplus = surplus - more
    return np.array(counts)


def normal_values(stream_key, extent, scale, reach, shards=(), held_as=jnp.bfloat16):
    result = scale * jax.random.normal(stream_key, extent, jnp.float32)
    if shards:
        result = result * level_of(stream_key, extent, shards, -0.22, 0.18)
    return jnp.clip(result, -reach, reach).astype(held_as)


def setup_inputs(seed: int = 0) -> dict:
    key_list = jax.random.split(jax.random.key(seed), 7)
    values = draw_values(jax.random.fold_in(key_list[6], 71), 0)
    subgroup = set_ends(jax.random.randint(key_list[1], (TILES,), 0, GRP_DEV), jax.random.fold_in(key_list[1], 1), 0, GRP_DEV - 1).astype(jnp.int32)
    owners_keys = jax.random.split(jax.random.fold_in(key_list[2], 1), TILES // TILES_DEV)
    owners_turns = jax.random.permutation(jax.random.fold_in(key_list[2], 3), TILES // TILES_DEV)
    owners = jax.vmap(lambda own, number: assign_block(jax.random.fold_in(key_list[2], 2), own, number, TILES_DEV, N_SHUF, 1, CAP, 1))(owners_keys, owners_turns).reshape((TILES, 1))
    col_gain = jnp.clip(1.0 + 0.1 * jax.random.normal(key_list[3], (COLS,), jnp.float32), 0.5, 1.5)
    col_bias = normal_values(key_list[4], (COLS,), 0.5, 3.0, ((0, 4),), jnp.float32)
    out_weight = normal_values(key_list[5], (COLS, OUT), COLS ** -0.5, 0.1875, ((0, 4),))
    return {"values": values, "subgroup": subgroup, "owners": owners, "col_gain": col_gain, "col_bias": col_bias, "out_weight": out_weight}


def reference(values, subgroup, owners, col_gain, col_bias, out_weight):
    row_total, col_total = values.shape
    tile_total = row_total // TILE
    groups = GRP_DEV * N_SHUF
    group = (owners[:, 0] * GRP_DEV + subgroup).astype(jnp.int32)
    shaped = values.astype(jnp.float32).reshape(tile_total, TILE, col_total)
    tile_sum = lax.optimization_barrier(jnp.sum(shaped, axis=1))
    tile_sq = lax.optimization_barrier(jnp.sum(shaped * shaped, axis=1))
    group_sum = jax.ops.segment_sum(tile_sum, group, num_segments=groups)
    group_sq = jax.ops.segment_sum(tile_sq, group, num_segments=groups)
    count = jax.ops.segment_sum(jnp.full((tile_total,), float(TILE), jnp.float32), group, num_segments=groups)
    mean_all = lax.optimization_barrier(jnp.sum(tile_sum, axis=0)) / float(row_total)
    square_all = lax.optimization_barrier(jnp.sum(tile_sq, axis=0)) / float(row_total)
    weight = (count + float(PRIOR))[:, None]
    center = (group_sum + float(PRIOR) * mean_all) / weight
    second = (group_sq + float(PRIOR) * square_all) / weight
    inverse = lax.rsqrt(second - center * center + 1e-05)
    tile_center = center[group]
    tile_scale = inverse[group] * col_gain
    scored = ((shaped - tile_center[:, None, :]) * tile_scale[:, None, :] + col_bias).astype(jnp.bfloat16)
    scored = scored.reshape(row_total, col_total)
    block_cols = col_total // N_REP
    summed = jnp.zeros((row_total, out_weight.shape[1]), jnp.float32)
    for block in range(N_REP):
        partial_value = jnp.dot(scored[:, block * block_cols:(block + 1) * block_cols], out_weight[block * block_cols:(block + 1) * block_cols], preferred_element_type=jnp.float32)
        summed = summed + partial_value.astype(jnp.bfloat16).astype(jnp.float32)
    return summed.astype(jnp.bfloat16)
```

```python
import functools
import math

import jax
import jax.numpy as jnp
from jax import lax
from jax.experimental import pallas as pl
from jax.experimental.pallas import tpu as pltpu
from jax.sharding import PartitionSpec as P

GRP_DEV = 32
PRIOR = 256
EPS = 1e-05
EXTRA = 8
EARLY = 8
PAIR = 2
PARTS = (4, 4, 8)
LIMIT = 58900 * 1024
LIMIT_LAST = 8 * 1024 * 1024
MESH = pl.DeviceIdType.MESH


def kernel(
    shuf_size,
    rep_size,
    early,
    values,
    weight,
    owner,
    member,
    gain,
    bias,
    out,
    last,
    weights,
    held,
    main,
    packets,
    stat,
    stats_in,
    rep_ready,
    shuf_ready,
    load_sem,
    own_sem,
    far_send,
    far_recv,
    near_send,
    near_recv,
    pack_send,
    pack_recv,
    fwd_send,
    fwd_recv,
    wx_send,
    wx_recv,
    wg_send,
    wg_recv,
    wf_send,
    wf_recv,
    wn_send,
    wn_recv,
    st_send,
    st_recv,
):
    shuf, rep = lax.axis_index("shuf"), lax.axis_index("rep")
    half = rep_size // 2
    outer = shuf_size // 2
    slices = weights.shape[2]
    slice_outer = slices // 2
    local_rows, cols = values.shape
    block_rows = local_rows // rep_size
    tiles = member.shape[1]
    tile_rows = local_rows // tiles
    block_tiles = tiles // rep_size
    main_rows = main.shape[0]
    main_tiles = main_rows // tile_rows
    high, low = rep // half, rep % half
    s_out, s_in = shuf // 2, shuf % 2
    mate = s_out * 2 + 1 - s_in
    cut = shuf % slices
    cut_base = shuf - cut
    cut_out = cut // 2

    def rep_peer(dh, dl):
        return ((high + dh) % 2) * half + (low + dl) % half

    def outer_peer(e):
        return ((s_out + e) % outer) * 2 + s_in

    def cut_peer(e):
        return cut_base + ((cut_out + e) % slice_outer) * 2 + s_in

    far = [(1, dl) for dl in range(half)]
    near = [(0, dl) for dl in range(1, half)]
    rep_offsets = near + far

    def remote(src, dst, send, recv, s, k):
        return pltpu.make_async_remote_copy(
            src_ref=src, dst_ref=dst, send_sem=send, recv_sem=recv,
            device_id=(s, k), device_id_type=MESH,
        )

    def held_rows(block, tile, count):
        start = pl.multiple_of((block * block_tiles + tile) * tile_rows, tile_rows)
        return pl.ds(start, count * tile_rows)

    def tile_at(tile):
        if isinstance(tile, int) and tile >= main_tiles:
            return last, pl.ds((tile - main_tiles) * tile_rows, tile_rows)
        return main, pl.ds(pl.multiple_of(tile * tile_rows, tile_rows), tile_rows)

    def slot_cols(dh, dl):
        slot = dh * half + dl
        return pl.ds(slot * cols, cols)

    def far_copy(dl, tile):
        peer = rep_peer(1, dl)
        dst, rows = tile_at(tile)
        return remote(
            held.at[held_rows(peer, tile, 1)], dst.at[rows, slot_cols(1, dl)],
            far_send.at[dl, tile], far_recv.at[dl, tile], shuf, peer,
        )

    def near_copy(dl, part):
        peer = rep_peer(0, dl)
        dst, tile = (main, 0) if part == 0 else (last, main_tiles)
        count = dst.shape[0] // tile_rows
        return remote(
            held.at[held_rows(peer, tile, count)], dst.at[:, slot_cols(0, dl)],
            near_send.at[dl, part], near_recv.at[dl, part], shuf, peer,
        )

    starts = [sum(PARTS[:i]) * block_tiles // sum(PARTS) for i in range(len(PARTS) + 1)]
    order = far + near + [(0, 0)]

    def load_copy(b, i):
        rows = held_rows(rep_peer(*order[b]), starts[i], starts[i + 1] - starts[i])
        return pltpu.make_async_copy(values.at[rows], held.at[rows], load_sem.at[b, i])

    own_weight = pltpu.make_async_copy(weight, weights.at[0, 0], own_sem)
    loads = [(b, i) for i in range(2) for b in range(half)]
    loads += [(b, i) for b in range(rep_size) for i in range(3) if (b, i) not in loads]
    for b, i in loads:
        load_copy(b, i).start()
    own_weight.start()

    barrier = pltpu.get_barrier_semaphore()
    leader, scout = low == half - 1, low == 0
    for dh, dl in rep_offsets:
        peer = rep_peer(dh, dl)

        @pl.when(peer % half == half - 1)
        def _():
            pl.semaphore_signal(barrier, inc=1, device_id=(shuf, peer), device_id_type=MESH)

    @pl.when(leader)
    def _():
        pl.semaphore_wait(barrier, rep_size - 1)
        for dl in range(1, half):
            pl.semaphore_signal(
                rep_ready, inc=1, device_id=(shuf, rep_peer(0, dl)), device_id_type=MESH
            )

    @pl.when(jnp.logical_not(leader))
    def _():
        pl.semaphore_wait(rep_ready, 1)

    waited = set()

    def load_wait(b, i):
        if (b, i) not in waited:
            waited.add((b, i))
            load_copy(b, i).wait()

    wx = remote(weight.at[cut], weights.at[1, 0, cut], wx_send, wx_recv, shuf, rep_peer(1, 0))
    sent = 0
    for i in range(len(PARTS)):
        if sent < early:
            for b in range(half):
                load_wait(b, i)
        while sent < min(early, starts[i + 1]):
            for dh, dl in far:
                far_copy(dl, sent).start()
            sent += 1
            if sent == 1:
                wx.start()

    shuf_peers = [mate] + [outer_peer(e) for e in range(1, outer)]

    @pl.when(scout)
    def _():
        for s in shuf_peers:
            pl.semaphore_signal(barrier, inc=1, device_id=(s, rep), device_id_type=MESH)
        pl.semaphore_wait(barrier, len(shuf_peers))
        for dl in range(1, half):
            pl.semaphore_signal(
                shuf_ready, inc=1, device_id=(shuf, rep_peer(0, dl)), device_id_type=MESH
            )

    @pl.when(jnp.logical_not(scout))
    def _():
        pl.semaphore_wait(shuf_ready, 1)

    gid_row = (owner[...] * GRP_DEV + member[...]).astype(jnp.float32)
    packets[0, 0, tiles:tiles + 1, :tiles] = gid_row
    square = (tiles, tiles)
    on_diagonal = lax.broadcasted_iota(jnp.int32, square, 0) == lax.broadcasted_iota(jnp.int32, square, 1)
    gid_col = jnp.sum(jnp.where(on_diagonal, gid_row, 0.0), axis=1, keepdims=True)
    gid_col = jnp.concatenate([gid_col, jnp.full((EXTRA, 1), -1.0, jnp.float32)], axis=0)
    group = 8
    for b in range(rep_size):
        block = rep_peer(*order[b])
        for g in range(block_tiles // group):
            for i in range(len(PARTS)):
                if starts[i] < (g + 1) * group:
                    load_wait(b, i)
            parts, squares = [], []
            for u in range(group):
                x = held[held_rows(block, g * group + u, 1), :].astype(jnp.float32)
                parts.append(jnp.sum(x, axis=0, keepdims=True))
                squares.append(jnp.sum(x * x, axis=0, keepdims=True))
            first = pl.multiple_of(block * block_tiles + g * group, group)
            packets[0, 0, pl.ds(first, group), :cols] = jnp.concatenate(parts, axis=0)
            packets[0, 0, pl.ds(first, group), cols:] = jnp.concatenate(squares, axis=0)

    def pack_copy(e):
        return remote(
            packets.at[0, 0], packets.at[0, e], pack_send.at[e], pack_recv.at[e], outer_peer(e), rep
        )

    def fwd_copy(e):
        return remote(
            packets.at[0, e], packets.at[1, e], fwd_send.at[e], fwd_recv.at[e], mate, rep
        )

    def cut_copy(e):
        here = weights.at[1, 0, cut]
        return remote(here, here, wg_send.at[e], wg_recv.at[e], cut_peer(e), rep)

    def cut_forward(e):
        index = ((cut_out + slice_outer - e) % slice_outer) * 2 + s_in
        there = weights.at[1, 0, index]
        return remote(there, there, wf_send.at[e], wf_recv.at[e], mate, rep)

    for e in range(1, outer):
        pack_copy(e).start()
    fwd_copy(0).start()
    wx.wait_recv()
    for e in range(1, slice_outer):
        cut_copy(e).start()

    def members(i, e):
        same = gid_col == packets[i, e, tiles:tiles + 1, :tiles]
        row = lax.broadcasted_iota(jnp.int32, (tiles + EXTRA, tiles), 0)
        return jnp.where(same | (row >= tiles), 1.0, 0.0).astype(jnp.float32)

    def gathered(i, e):
        m = members(i, e)
        part = jnp.dot(
            m, packets[i, e, :tiles, :],
            precision=lax.Precision.HIGHEST, preferred_element_type=jnp.float32,
        )
        return part, jnp.sum(m, axis=1, keepdims=True)

    total, count = gathered(0, 0)
    for e in range(1, outer):
        pack_copy(e).wait_recv()
        fwd_copy(e).start()
        part, number = gathered(0, e)
        total, count = total + part, count + number
    cut_forward(0).start()
    for e in range(1, slice_outer):
        cut_copy(e).wait_recv()
        cut_forward(e).start()
    for e in range(outer):
        fwd_copy(e).wait_recv()
        part, number = gathered(1, e)
        total, count = total + part, count + number

    row_count = float(local_rows * shuf_size)
    overall = total[tiles:tiles + 1] / row_count
    weight_sum = count[:tiles] * float(tile_rows) + float(PRIOR)
    pooled = (total[:tiles] + float(PRIOR) * overall) / weight_sum
    center, second = pooled[:, :cols], pooled[:, cols:]
    scale = lax.rsqrt(second - center * center + EPS) * gain[...]
    stat[0] = scale
    stat[1] = bias[...] - center * scale

    def stat_copy(dl):
        peer = rep_peer(1, dl)
        rows = pl.ds(pl.multiple_of(peer * block_tiles, 8), stats_in.shape[2])
        return remote(
            stat.at[:, rows], stats_in.at[dl], st_send.at[dl], st_recv.at[dl], shuf, peer
        )

    for dh, dl in far:
        stat_copy(dl).start()

    def scored(block, tile):
        x = held[held_rows(block, tile, 1), :].astype(jnp.float32)
        at = pl.ds(block * block_tiles + tile, 1)
        return (x * stat[0, at, :] + stat[1, at, :]).astype(jnp.bfloat16)

    def late(tile):
        for dh, dl in far:
            peer = rep_peer(dh, dl)
            held[held_rows(peer, tile, 1), :] = scored(peer, tile)
            far_copy(dl, tile).start()

    def late_step(tile, carry):
        late(tile)
        return carry

    lax.fori_loop(early, main_tiles, late_step, 0)
    for tile in range(main_tiles, block_tiles):
        late(tile)

    def near_step(tile, carry):
        for dh, dl in near:
            peer = rep_peer(dh, dl)
            held[held_rows(peer, tile, 1), :] = scored(peer, tile)
        return carry

    lax.fori_loop(0, block_tiles, near_step, 0)
    for dh, dl in near:
        for part in range(2):
            near_copy(dl, part).start()

    def own_step(tile, carry):
        dst, rows = tile_at(tile)
        dst[rows, :cols] = scored(rep, tile)
        return carry

    lax.fori_loop(0, main_tiles, own_step, 0)
    for tile in range(main_tiles, block_tiles):
        own_step(tile, 0)

    own_weight.wait()
    for e in range(slice_outer):
        cut_forward(e).wait_recv()

    def share_copy(dh, dl):
        return remote(
            weights.at[dh, 0], weights.at[dh, dl],
            wn_send.at[dh, dl], wn_recv.at[dh, dl], shuf, rep_peer(0, dl),
        )

    for dl in range(1, half):
        for dh in range(2):
            share_copy(dh, dl).start()
    for dh, dl in far:
        stat_copy(dl).wait_recv()

    def early_step(tile, carry):
        dst, rows = tile_at(tile)
        for dh, dl in far:
            far_copy(dl, tile).wait_recv()
            at = slot_cols(dh, dl)
            x = dst[rows, at].astype(jnp.float32)
            s = stats_in[dl, 0, pl.ds(tile, 1), :]
            t = stats_in[dl, 1, pl.ds(tile, 1), :]
            dst[rows, at] = (x * s + t).astype(jnp.bfloat16)
        return carry

    lax.fori_loop(0, early, early_step, 0)
    for dl in range(1, half):
        for dh in range(2):
            share_copy(dh, dl).wait_recv()
    for dh, dl in near:
        for part in range(2):
            near_copy(dl, part).wait_recv()

    def project(pair, carry):
        for u in range(PAIR):
            tile = pair * PAIR + u

            @pl.when(tile >= early)
            def _():
                for dh, dl in far:
                    far_copy(dl, tile).wait_recv()

        size = PAIR * tile_rows
        rows = pl.ds(pl.multiple_of(pair * size, size), size)
        whole = weights[...].reshape(rep_size * cols, weights.shape[-1])
        out[rows, :] = jnp.dot(
            main[rows, :], whole, preferred_element_type=jnp.float32
        ).astype(out.dtype)
        return carry

    lax.fori_loop(0, main_tiles // PAIR, project, 0)

    wx.wait_send()
    for e in range(1, outer):
        pack_copy(e).wait_send()
    for e in range(outer):
        fwd_copy(e).wait_send()
    for e in range(1, slice_outer):
        cut_copy(e).wait_send()
    for e in range(slice_outer):
        cut_forward(e).wait_send()
    for dh, dl in far:
        stat_copy(dl).wait_send()
    for dl in range(1, half):
        for dh in range(2):
            share_copy(dh, dl).wait_send()
    for dh, dl in near:
        for part in range(2):
            near_copy(dl, part).wait_send()
    for tile in range(block_tiles):
        for dh, dl in far:
            far_copy(dl, tile).wait_send()
    for tile in range(main_tiles, block_tiles):
        for dh, dl in far:
            far_copy(dl, tile).wait_recv()


def finish(early, scored, weights, out, tail, sems):
    rows, size = early.shape[0], scored.shape[0]
    count = rows // size

    def early_copy(i):
        return pltpu.make_async_copy(
            early.at[pl.ds(i * size, size)], out.at[pl.ds(i * size, size)], sems.at[i]
        )

    for i in range(count):
        early_copy(i).start()
    whole = weights[...].reshape(scored.shape[1], weights.shape[-1])
    tail[...] = jnp.dot(scored[...], whole, preferred_element_type=jnp.float32).astype(tail.dtype)
    tail_copy = pltpu.make_async_copy(tail, out.at[pl.ds(rows, size)], sems.at[count])
    tail_copy.start()
    for i in range(count):
        early_copy(i).wait()
    tail_copy.wait()


def on_device(shuf_size, rep_size, values, subgroup, owners, col_gain, col_bias, out_weight):
    local_rows, cols = values.shape
    tiles = subgroup.shape[0]
    outs = out_weight.shape[1]
    slices = math.gcd(shuf_size, cols // 32)
    outer, half, slice_outer = shuf_size // 2, rep_size // 2, slices // 2
    block_rows = local_rows // rep_size
    block_tiles = tiles // rep_size
    final = PAIR * local_rows // tiles
    early = block_tiles * EARLY // 16
    f32, bf16 = jnp.float32, jnp.bfloat16
    dma = pltpu.SemaphoreType.DMA
    vmem = pl.BlockSpec(memory_space=pltpu.VMEM)
    hbm = pl.BlockSpec(memory_space=pltpu.HBM)
    first, last, weights = pl.pallas_call(
        functools.partial(kernel, shuf_size, rep_size, early),
        out_shape=(
            pltpu.VMEM((block_rows - final, outs), bf16),
            pltpu.VMEM((final, rep_size * cols), bf16),
            pltpu.VMEM((2, half, slices, cols // slices, outs), bf16),
        ),
        in_specs=[hbm, hbm, vmem, vmem, vmem, vmem],
        out_specs=(vmem, vmem, vmem),
        scratch_shapes=[
            pltpu.VMEM((local_rows, cols), bf16),
            pltpu.VMEM((block_rows - final, rep_size * cols), bf16),
            pltpu.VMEM((2, outer, tiles + EXTRA, 2 * cols), f32),
            pltpu.VMEM((2, tiles, cols), f32),
            pltpu.VMEM((half, 2, -(-early // 8) * 8, cols), f32),
            pltpu.SemaphoreType.REGULAR,
            pltpu.SemaphoreType.REGULAR,
            dma((rep_size, len(PARTS))),
            dma,
            dma((half, block_tiles)),
            dma((half, block_tiles)),
            dma((half, 2)),
            dma((half, 2)),
            dma((outer,)),
            dma((outer,)),
            dma((outer,)),
            dma((outer,)),
            dma,
            dma,
            dma((slice_outer,)),
            dma((slice_outer,)),
            dma((slice_outer,)),
            dma((slice_outer,)),
            dma((2, half)),
            dma((2, half)),
            dma((half,)),
            dma((half,)),
        ],
        compiler_params=pltpu.CompilerParams(
            collective_id=0, has_side_effects=True, vmem_limit_bytes=LIMIT
        ),
    )(
        values,
        out_weight.reshape(slices, cols // slices, outs),
        owners.reshape(1, tiles),
        subgroup.reshape(1, tiles),
        col_gain[None, :],
        col_bias[None, :],
    )
    return pl.pallas_call(
        finish,
        out_shape=jax.ShapeDtypeStruct((block_rows, outs), bf16),
        in_specs=[vmem, vmem, vmem],
        out_specs=hbm,
        scratch_shapes=[pltpu.VMEM((final, outs), bf16), dma((block_rows // final,))],
        compiler_params=pltpu.CompilerParams(vmem_limit_bytes=LIMIT_LAST),
    )(first, last, weights)


def solution(mesh):
    return jax.shard_map(
        functools.partial(on_device, mesh.shape["shuf"], mesh.shape["rep"]),
        mesh=mesh,
        in_specs=(P("shuf", "rep"), P("shuf"), P("shuf", None), P("rep"), P("rep"), P("rep", None)),
        out_specs=P(("shuf", "rep"), None),
        check_vma=False,
    )
```

```python
import functools
import math

import jax
import jax.numpy as jnp
from jax import lax
from jax.experimental import pallas as pl
from jax.experimental.pallas import tpu as pltpu
from jax.sharding import PartitionSpec as P

GRP_DEV = 32
PRIOR = 256
EPS = 1e-05
EXTRA = 8
EARLY = 8
PAIR = 2
PARTS = (4, 4, 8)
LIMIT = 58900 * 1024
LIMIT_LAST = 8 * 1024 * 1024
MESH = pl.DeviceIdType.MESH


def kernel(
    shuf_size,
    rep_size,
    early,
    values,
    weight,
    owner_hbm,
    member_hbm,
    gain_hbm,
    bias_hbm,
    out,
    last,
    weights,
    held,
    main,
    packets,
    spreads,
    owner,
    member,
    gain,
    bias,
    stat,
    stats_out,
    stats_in,
    rep_ready,
    shuf_ready,
    load_sem,
    own_sem,
    small_sem,
    far_send,
    far_recv,
    near_send,
    near_recv,
    pack_send,
    pack_recv,
    spread_send,
    spread_recv,
    fwd_send,
    fwd_recv,
    over_send,
    over_recv,
    wx_send,
    wx_recv,
    wg_send,
    wg_recv,
    wf_send,
    wf_recv,
    wn_send,
    wn_recv,
    st_send,
    st_recv,
):
    shuf, rep = lax.axis_index("shuf"), lax.axis_index("rep")
    half = rep_size // 2
    outer = shuf_size // 2
    slices = weights.shape[2]
    slice_outer = slices // 2
    local_rows, cols = values.shape
    block_rows = local_rows // rep_size
    tiles = member.shape[1]
    tile_rows = local_rows // tiles
    block_tiles = tiles // rep_size
    main_rows = main.shape[0]
    main_tiles = main_rows // tile_rows
    high, low = rep // half, rep % half
    s_out, s_in = shuf // 2, shuf % 2
    mate = s_out * 2 + 1 - s_in
    cut = shuf % slices
    cut_base = shuf - cut
    cut_out = cut // 2

    def rep_peer(dh, dl):
        return ((high + dh) % 2) * half + (low + dl) % half

    def outer_peer(e):
        return ((s_out + e) % outer) * 2 + s_in

    def cut_peer(e):
        return cut_base + ((cut_out + e) % slice_outer) * 2 + s_in

    far = [(1, dl) for dl in range(half)]
    near = [(0, dl) for dl in range(1, half)]
    rep_offsets = near + far

    def remote(src, dst, send, recv, s, k):
        return pltpu.make_async_remote_copy(
            src_ref=src, dst_ref=dst, send_sem=send, recv_sem=recv,
            device_id=(s, k), device_id_type=MESH,
        )

    def held_rows(block, tile, count):
        start = pl.multiple_of((block * block_tiles + tile) * tile_rows, tile_rows)
        return pl.ds(start, count * tile_rows)

    def tile_at(tile):
        if isinstance(tile, int) and tile >= main_tiles:
            return last, pl.ds((tile - main_tiles) * tile_rows, tile_rows)
        return main, pl.ds(pl.multiple_of(tile * tile_rows, tile_rows), tile_rows)

    def slot_cols(dh, dl):
        slot = dh * half + dl
        return pl.ds(slot * cols, cols)

    def far_copy(dl, tile):
        peer = rep_peer(1, dl)
        dst, rows = tile_at(tile)
        return remote(
            held.at[held_rows(peer, tile, 1)], dst.at[rows, slot_cols(1, dl)],
            far_send.at[dl, tile], far_recv.at[dl, tile], shuf, peer,
        )

    def near_copy(dl, part):
        peer = rep_peer(0, dl)
        dst, tile = (main, 0) if part == 0 else (last, main_tiles)
        count = dst.shape[0] // tile_rows
        return remote(
            held.at[held_rows(peer, tile, count)], dst.at[:, slot_cols(0, dl)],
            near_send.at[dl, part], near_recv.at[dl, part], shuf, peer,
        )

    starts = [sum(PARTS[:i]) * block_tiles // sum(PARTS) for i in range(len(PARTS) + 1)]
    order = far + near + [(0, 0)]

    def load_copy(b, i):
        rows = held_rows(rep_peer(*order[b]), starts[i], starts[i + 1] - starts[i])
        return pltpu.make_async_copy(values.at[rows], held.at[rows], load_sem.at[b, i])

    own_weight = pltpu.make_async_copy(weight, weights.at[0, 0], own_sem)
    loads = [(b, i) for i in range(2) for b in range(half)]
    loads += [(b, i) for b in range(rep_size) for i in range(3) if (b, i) not in loads]
    barrier = pltpu.get_barrier_semaphore()
    leader, scout = low == half - 1, low == 0
    for dh, dl in rep_offsets:
        peer = rep_peer(dh, dl)

        @pl.when(peer % half == half - 1)
        def _():
            pl.semaphore_signal(barrier, inc=1, device_id=(shuf, peer), device_id_type=MESH)

    for b, i in loads:
        load_copy(b, i).start()
    small = [
        pltpu.make_async_copy(src, dst, small_sem.at[i])
        for i, (src, dst) in enumerate(
            [(owner_hbm, owner), (member_hbm, member), (gain_hbm, gain), (bias_hbm, bias)]
        )
    ]
    for copy in small:
        copy.start()
    own_weight.start()

    @pl.when(leader)
    def _():
        pl.semaphore_wait(barrier, rep_size - 1)
        for dl in range(1, half):
            pl.semaphore_signal(
                rep_ready, inc=1, device_id=(shuf, rep_peer(0, dl)), device_id_type=MESH
            )

    @pl.when(jnp.logical_not(leader))
    def _():
        pl.semaphore_wait(rep_ready, 1)

    waited = set()

    def load_wait(b, i):
        if (b, i) not in waited:
            waited.add((b, i))
            load_copy(b, i).wait()

    wx = remote(weight.at[cut], weights.at[1, 0, cut], wx_send, wx_recv, shuf, rep_peer(1, 0))
    sent = 0
    for i in range(len(PARTS)):
        if sent < early:
            for b in range(half):
                load_wait(b, i)
        while sent < min(early, starts[i + 1]):
            for dh, dl in far:
                far_copy(dl, sent).start()
            sent += 1
            if sent == 1:
                wx.start()

    shuf_peers = [mate] + [outer_peer(e) for e in range(1, outer)]

    @pl.when(scout)
    def _():
        for s in shuf_peers:
            pl.semaphore_signal(barrier, inc=1, device_id=(s, rep), device_id_type=MESH)
        pl.semaphore_wait(barrier, len(shuf_peers))
        for dl in range(1, half):
            pl.semaphore_signal(
                shuf_ready, inc=1, device_id=(shuf, rep_peer(0, dl)), device_id_type=MESH
            )

    @pl.when(jnp.logical_not(scout))
    def _():
        pl.semaphore_wait(shuf_ready, 1)

    for copy in small:
        copy.wait()
    gid_row = (owner[...] * GRP_DEV + member[...]).astype(jnp.float32)
    packets[0, 0, tiles:tiles + 1, :tiles] = gid_row
    square = (tiles, tiles)
    on_diagonal = lax.broadcasted_iota(jnp.int32, square, 0) == lax.broadcasted_iota(jnp.int32, square, 1)
    gid_col = jnp.sum(jnp.where(on_diagonal, gid_row, 0.0), axis=1, keepdims=True)
    gid_col = jnp.concatenate([gid_col, jnp.full((EXTRA, 1), -1.0, jnp.float32)], axis=0)
    group = 8
    for b in range(rep_size):
        block = rep_peer(*order[b])
        spread_rows = []
        for g in range(block_tiles // group):
            for i in range(len(PARTS)):
                if starts[i] < (g + 1) * group:
                    load_wait(b, i)
            parts, squares = [], []
            for u in range(group):
                x = held[held_rows(block, g * group + u, 1), :].astype(jnp.float32)
                parts.append(jnp.sum(x, axis=0, keepdims=True))
                squares.append(jnp.sum(x * x, axis=0, keepdims=True))
            first = pl.multiple_of(block * block_tiles + g * group, group)
            part = jnp.concatenate(parts, axis=0)
            spread = jnp.concatenate(squares, axis=0) - part * part * (1.0 / tile_rows)
            packets[0, 0, pl.ds(first, group), :] = part
            spread_rows.append(spread.astype(jnp.bfloat16))
        at = pl.ds(pl.multiple_of(block * block_tiles, block_tiles), block_tiles)
        spreads[0, 0, at, :] = jnp.concatenate(spread_rows, axis=0)

    def pack_copies(e):
        to = outer_peer(e), rep
        return [
            remote(packets.at[0, 0], packets.at[0, e], pack_send.at[e], pack_recv.at[e], *to),
            remote(spreads.at[0, 0], spreads.at[0, e], spread_send.at[e], spread_recv.at[e], *to),
        ]

    def fwd_copies(e):
        to = mate, rep
        return [
            remote(packets.at[0, e], packets.at[1, e], fwd_send.at[e], fwd_recv.at[e], *to),
            remote(spreads.at[0, e], spreads.at[1, e], over_send.at[e], over_recv.at[e], *to),
        ]

    def start(copies):
        for copy in copies:
            copy.start()

    def received(copies):
        for copy in copies:
            copy.wait_recv()

    def cut_copy(e):
        here = weights.at[1, 0, cut]
        return remote(here, here, wg_send.at[e], wg_recv.at[e], cut_peer(e), rep)

    def cut_forward(e):
        index = ((cut_out + slice_outer - e) % slice_outer) * 2 + s_in
        there = weights.at[1, 0, index]
        return remote(there, there, wf_send.at[e], wf_recv.at[e], mate, rep)

    for e in range(1, outer):
        start(pack_copies(e))
    start(fwd_copies(0))

    def members(i, e):
        same = gid_col == packets[i, e, tiles:tiles + 1, :tiles]
        row = lax.broadcasted_iota(jnp.int32, (tiles + EXTRA, tiles), 0)
        return jnp.where(same | (row >= tiles), 1.0, 0.0).astype(jnp.float32)

    def gathered(i, e):
        m = members(i, e)
        sums = packets[i, e, :tiles, :]
        squares = spreads[i, e].astype(jnp.float32) + sums * sums * (1.0 / tile_rows)
        part = jnp.dot(
            m, jnp.concatenate([sums, squares], axis=1),
            precision=lax.Precision.HIGHEST, preferred_element_type=jnp.float32,
        )
        return part, jnp.sum(m, axis=1, keepdims=True)

    total, count = gathered(0, 0)
    for e in range(1, outer):
        received(pack_copies(e))
        start(fwd_copies(e))
        part, number = gathered(0, e)
        total, count = total + part, count + number
    wx.wait_recv()
    for e in range(1, slice_outer):
        cut_copy(e).start()
    cut_forward(0).start()
    for e in range(outer):
        received(fwd_copies(e))
        part, number = gathered(1, e)
        total, count = total + part, count + number

    row_count = float(local_rows * shuf_size)
    overall = total[tiles:tiles + 1] / row_count
    weight_sum = count[:tiles] * float(tile_rows) + float(PRIOR)
    pooled = (total[:tiles] + float(PRIOR) * overall) / weight_sum
    center, second = pooled[:, :cols], pooled[:, cols:]
    scale = lax.rsqrt(second - center * center + EPS) * gain[...]
    stat[0] = scale
    stat[1] = bias[...] - center * scale

    def stat_copy(dl):
        return remote(
            stats_out.at[dl], stats_in.at[dl], st_send.at[dl], st_recv.at[dl], shuf, rep_peer(1, dl)
        )

    for dh, dl in far:
        at = pl.ds(pl.multiple_of(rep_peer(dh, dl) * block_tiles, block_tiles), block_tiles)
        for k in range(2):
            stats_out[dl, k * early:(k + 1) * early, :] = stat[k, at, :][:early]
        stat_copy(dl).start()

    def scored(block, tile):
        x = held[held_rows(block, tile, 1), :].astype(jnp.float32)
        at = pl.ds(block * block_tiles + tile, 1)
        return (x * stat[0, at, :] + stat[1, at, :]).astype(jnp.bfloat16)

    def late(tile):
        for dh, dl in far:
            peer = rep_peer(dh, dl)
            held[held_rows(peer, tile, 1), :] = scored(peer, tile)
            far_copy(dl, tile).start()

    def late_step(tile, carry):
        late(tile)
        return carry

    lax.fori_loop(early, main_tiles, late_step, 0)
    for tile in range(main_tiles, block_tiles):
        late(tile)

    for e in range(1, slice_outer):
        cut_copy(e).wait_recv()
        cut_forward(e).start()

    def near_step(tile, carry):
        for dh, dl in near:
            peer = rep_peer(dh, dl)
            held[held_rows(peer, tile, 1), :] = scored(peer, tile)
        return carry

    lax.fori_loop(0, block_tiles, near_step, 0)
    for dh, dl in near:
        for part in range(2):
            near_copy(dl, part).start()

    def own_step(tile, carry):
        dst, rows = tile_at(tile)
        dst[rows, :cols] = scored(rep, tile)
        return carry

    lax.fori_loop(0, main_tiles, own_step, 0)
    for tile in range(main_tiles, block_tiles):
        own_step(tile, 0)

    own_weight.wait()
    for e in range(slice_outer):
        cut_forward(e).wait_recv()

    def share_copy(dh, dl):
        return remote(
            weights.at[dh, 0], weights.at[dh, dl],
            wn_send.at[dh, dl], wn_recv.at[dh, dl], shuf, rep_peer(0, dl),
        )

    for dl in range(1, half):
        for dh in range(2):
            share_copy(dh, dl).start()
    for dh, dl in far:
        stat_copy(dl).wait_recv()

    def early_step(tile, carry):
        dst, rows = tile_at(tile)
        for dh, dl in far:
            far_copy(dl, tile).wait_recv()
            at = slot_cols(dh, dl)
            x = dst[rows, at].astype(jnp.float32)
            s = stats_in[dl, pl.ds(tile, 1), :]
            t = stats_in[dl, pl.ds(early + tile, 1), :]
            dst[rows, at] = (x * s + t).astype(jnp.bfloat16)
        return carry

    lax.fori_loop(0, early, early_step, 0)
    for dl in range(1, half):
        for dh in range(2):
            share_copy(dh, dl).wait_recv()
    for dh, dl in near:
        for part in range(2):
            near_copy(dl, part).wait_recv()

    def project(pair, carry):
        for u in range(PAIR):
            tile = pair * PAIR + u

            @pl.when(tile >= early)
            def _():
                for dh, dl in far:
                    far_copy(dl, tile).wait_recv()

        size = PAIR * tile_rows
        rows = pl.ds(pl.multiple_of(pair * size, size), size)
        whole = weights[...].reshape(rep_size * cols, weights.shape[-1])
        out[rows, :] = jnp.dot(
            main[rows, :], whole, preferred_element_type=jnp.float32
        ).astype(out.dtype)
        return carry

    lax.fori_loop(0, main_tiles // PAIR, project, 0)

    wx.wait_send()
    for e in range(1, outer):
        for copy in pack_copies(e):
            copy.wait_send()
    for e in range(outer):
        for copy in fwd_copies(e):
            copy.wait_send()
    for e in range(1, slice_outer):
        cut_copy(e).wait_send()
    for e in range(slice_outer):
        cut_forward(e).wait_send()
    for dh, dl in far:
        stat_copy(dl).wait_send()
    for dl in range(1, half):
        for dh in range(2):
            share_copy(dh, dl).wait_send()
    for dh, dl in near:
        for part in range(2):
            near_copy(dl, part).wait_send()
    for tile in range(block_tiles):
        for dh, dl in far:
            far_copy(dl, tile).wait_send()
    for tile in range(main_tiles, block_tiles):
        for dh, dl in far:
            far_copy(dl, tile).wait_recv()


def finish(early, scored, weights, out, tail, sems):
    rows, size = early.shape[0], scored.shape[0]
    count = rows // size

    def early_copy(i):
        return pltpu.make_async_copy(
            early.at[pl.ds(i * size, size)], out.at[pl.ds(i * size, size)], sems.at[i]
        )

    for i in range(count):
        early_copy(i).start()
    whole = weights[...].reshape(scored.shape[1], weights.shape[-1])
    tail[...] = jnp.dot(scored[...], whole, preferred_element_type=jnp.float32).astype(tail.dtype)
    tail_copy = pltpu.make_async_copy(tail, out.at[pl.ds(rows, size)], sems.at[count])
    tail_copy.start()
    for i in range(count):
        early_copy(i).wait()
    tail_copy.wait()


def on_device(shuf_size, rep_size, values, subgroup, owners, col_gain, col_bias, out_weight):
    local_rows, cols = values.shape
    tiles = subgroup.shape[0]
    outs = out_weight.shape[1]
    slices = math.gcd(shuf_size, cols // 32)
    outer, half, slice_outer = shuf_size // 2, rep_size // 2, slices // 2
    block_rows = local_rows // rep_size
    block_tiles = tiles // rep_size
    final = PAIR * local_rows // tiles
    early = block_tiles * EARLY // 16
    f32, bf16 = jnp.float32, jnp.bfloat16
    dma = pltpu.SemaphoreType.DMA
    vmem = pl.BlockSpec(memory_space=pltpu.VMEM)
    hbm = pl.BlockSpec(memory_space=pltpu.HBM)
    first, last, weights = pl.pallas_call(
        functools.partial(kernel, shuf_size, rep_size, early),
        out_shape=(
            pltpu.VMEM((block_rows - final, outs), bf16),
            pltpu.VMEM((final, rep_size * cols), bf16),
            pltpu.VMEM((2, half, slices, cols // slices, outs), bf16),
        ),
        in_specs=[hbm] * 6,
        out_specs=(vmem, vmem, vmem),
        scratch_shapes=[
            pltpu.VMEM((local_rows, cols), bf16),
            pltpu.VMEM((block_rows - final, rep_size * cols), bf16),
            pltpu.VMEM((2, outer, tiles + EXTRA, cols), f32),
            pltpu.VMEM((2, outer, tiles, cols), bf16),
            pltpu.VMEM((1, tiles), jnp.int32),
            pltpu.VMEM((1, tiles), jnp.int32),
            pltpu.VMEM((1, cols), f32),
            pltpu.VMEM((1, cols), f32),
            pltpu.VMEM((2, tiles, cols), f32),
            pltpu.VMEM((half, -(-2 * early // 8) * 8, cols), f32),
            pltpu.VMEM((half, -(-2 * early // 8) * 8, cols), f32),
            pltpu.SemaphoreType.REGULAR,
            pltpu.SemaphoreType.REGULAR,
            dma((rep_size, len(PARTS))),
            dma,
            dma((4,)),
            dma((half, block_tiles)),
            dma((half, block_tiles)),
            dma((half, 2)),
            dma((half, 2)),
            dma((outer,)),
            dma((outer,)),
            dma((outer,)),
            dma((outer,)),
            dma((outer,)),
            dma((outer,)),
            dma((outer,)),
            dma((outer,)),
            dma,
            dma,
            dma((slice_outer,)),
            dma((slice_outer,)),
            dma((slice_outer,)),
            dma((slice_outer,)),
            dma((2, half)),
            dma((2, half)),
            dma((half,)),
            dma((half,)),
        ],
        compiler_params=pltpu.CompilerParams(
            collective_id=0, has_side_effects=True, vmem_limit_bytes=LIMIT
        ),
    )(
        values,
        out_weight.reshape(slices, cols // slices, outs),
        owners.reshape(1, tiles),
        subgroup.reshape(1, tiles),
        col_gain[None, :],
        col_bias[None, :],
    )
    return pl.pallas_call(
        finish,
        out_shape=jax.ShapeDtypeStruct((block_rows, outs), bf16),
        in_specs=[vmem, vmem, vmem],
        out_specs=hbm,
        scratch_shapes=[pltpu.VMEM((final, outs), bf16), dma((block_rows // final,))],
        compiler_params=pltpu.CompilerParams(vmem_limit_bytes=LIMIT_LAST),
    )(first, last, weights)


def solution(mesh):
    return jax.shard_map(
        functools.partial(on_device, mesh.shape["shuf"], mesh.shape["rep"]),
        mesh=mesh,
        in_specs=(P("shuf", "rep"), P("shuf"), P("shuf", None), P("rep"), P("rep"), P("rep", None)),
        out_specs=P(("shuf", "rep"), None),
        check_vma=False,
    )
```
